32 devices in a mesh: frame: 32 (over z, y, x, core), segment: 1.
Axes of the slice: x: 2, y: 2, z: 4, core: 2. Of those that a mesh axis runs over, the one named last changes fastest.
Arguments:
- state: bfloat16 [1, 1024, 3072], P('segment', 'frame'), may hold values from -6 to 6
- modulation: float32 [1, 32, 7, 3072], P('segment'), may hold values from -3 to 3
- noise_level: int32 [4], replicated, may hold values from 0 to 31
- frame_mask: int32 [4, 4], replicated, may hold values from 0 to 1, as said below
- offset: int32 [1], replicated, may hold values from 1 to 3
Outputs:
- next_state: bfloat16 [1, 1024, 3072], P('segment', 'frame')
The draws below stay inside these ranges and needn't reach their ends.
Inputs may be any that keep to these rules, and one draw needn't show every extreme that they name: frame_mask[i, i] is 1 and frame_mask[i, j] is 0 for j > i.
All inputs are finite; a program needn't handle non-finite values.
Results may differ from the reference program's by a relative error of at most 0.017.
Values may be sent and summed in bfloat16 or wider, within the bound.
A program may use at most 128 MiB of HBM per device.

```python
import math
import jax
import jax.numpy as jnp
from jax import lax

D = 3072
HEADS = 24
HEAD = 128
LEVELS = 32
FRAME_TOK = 256
FRAMES = 4
TOKENS = 1024
N_SEGMENT = 1


def draw_frame_mask(key, part):
    frames_all = TOKENS // FRAME_TOK
    picks = jax.random.randint(jax.random.fold_in(key, 17), (frames_all, frames_all), 0, 4)
    row_ids = jnp.arange(frames_all, dtype=jnp.int32)[:, None]
    col_ids = jnp.arange(frames_all, dtype=jnp.int32)[None, :]
    earlier = jnp.where(picks > 0, 1, 0)
    return jnp.where(row_ids > col_ids, earlier, jnp.where(row_ids == col_ids, 1, 0)).astype(jnp.int32)


def draw_state(key, part):
    frames_all = TOKENS // FRAME_TOK
    background_share = 0.3
    carry_rate = 0.4 ** (1.0 / frames_all)
    fresh = jax.random.normal(jax.random.fold_in(key, 5), (N_SEGMENT, frames_all, FRAME_TOK * D), jnp.float32)
    frame_ids = jnp.arange(frames_all, dtype=jnp.int32)
    lag = frame_ids[:, None] - frame_ids[None, :]
    lag_float = jnp.maximum(lag, 0).astype(jnp.float32)
    entry_scale = jnp.where(frame_ids[None, :] == 0, 1.0, math.sqrt(1.0 - carry_rate * carry_rate))
    mixing = jnp.where(lag >= 0, jnp.power(jnp.float32(carry_rate), lag_float) * entry_scale, 0.0).astype(jnp.float32)
    carried = jnp.einsum('fg,sgc->sfc', mixing, fresh, precision=lax.Precision.HIGHEST)
    carried = carried.reshape(N_SEGMENT, frames_all, FRAME_TOK, D)
    backdrop = jax.random.normal(jax.random.fold_in(key, 9), (N_SEGMENT, D), jnp.float32)
    backdrop = backdrop / jnp.sqrt(jnp.mean(backdrop * backdrop, axis=-1, keepdims=True))
    framed = math.sqrt(background_share) * backdrop[:, None, None, :] + math.sqrt(1.0 - background_share) * carried
    noise_field = framed.reshape(N_SEGMENT, TOKENS, D)
    return jnp.clip(noise_field, -6.0, 6.0).astype(jnp.bfloat16)


def with_ends(drawn, key, low, high):
    shape = drawn.shape
    spot = [jax.random.randint(jax.random.fold_in(key, axis), (), 0, shape[axis]) for axis in range(len(shape))]
    drawn = drawn.at[tuple(spot)].set(low)
    longest = shape.index(max(shape))
    spot[longest] = (spot[longest] + 1) % shape[longest]
    return drawn.at[tuple(spot)].set(high)


def gaussian(stream_key, extent, spread, reach, kind=jnp.bfloat16):
    drawn = jax.random.normal(stream_key, extent, jnp.float32) * spread
    return jnp.minimum(jnp.maximum(drawn, -reach), reach).astype(kind)


def setup_inputs(seed: int = 0) -> dict:
    keys = jax.random.split(jax.random.key(seed), 6)
    return {
        "state": draw_state(jax.random.fold_in(keys[5], 71), 0),
        "modulation": gaussian(keys[1], (N_SEGMENT, LEVELS, 7, D), 0.5, 3.0, jnp.float32),
        "noise_level": with_ends(jax.random.randint(keys[2], (FRAMES,), 0, LEVELS), jax.random.fold_in(keys[2], 1), 0, LEVELS - 1).astype(jnp.int32),
        "frame_mask": draw_frame_mask(jax.random.fold_in(keys[5], 71), 0),
        "offset": jax.random.randint(keys[4], (1,), 1, FRAMES).astype(jnp.int32),
    }


epsilon = 1e-06

def normalize(values):
    widened = values.astype(jnp.float32)
    square_mean = lax.optimization_barrier(jnp.mean(widened * widened, axis=-1, keepdims=True))
    return (widened * lax.rsqrt(square_mean + epsilon)).astype(jnp.bfloat16)

def modulate(normed, modifiers, column):
    scaled = normed.astype(jnp.float32) * (1.0 + modifiers[:, column]) + modifiers[:, column + 1]
    return scaled.astype(jnp.bfloat16)

def section(hidden, level_table, noise_level, frame_mask):
    tokens_all = hidden.shape[0]
    row_frames = jnp.arange(tokens_all, dtype=jnp.int32) // FRAME_TOK
    modifiers = level_table[noise_level[row_frames]]
    normed = normalize(hidden)
    queries = modulate(normed, modifiers, 0)
    keys_all = modulate(normed, modifiers, 2)
    values_all = modulate(normed, modifiers, 4)
    allowed = frame_mask[row_frames][:, row_frames] == 1
    scale_factor = 1.0 / math.sqrt(HEAD)

    def split_heads(rows):
        return jnp.transpose(rows.reshape(tokens_all, HEADS, HEAD), (1, 0, 2))

    def per_head(stacked):
        query_head, key_head, value_head = stacked
        scores = jnp.dot(query_head, key_head.T, preferred_element_type=jnp.float32) * scale_factor
        scores = jnp.where(allowed, scores, jnp.float32(-1e+30))
        row_max = lax.optimization_barrier(jnp.max(scores, axis=-1, keepdims=True))
        weights = jnp.where(allowed, jnp.exp(scores - row_max), jnp.float32(0.0)).astype(jnp.bfloat16)
        summed = jnp.dot(weights, value_head, preferred_element_type=jnp.float32)
        denominator = lax.optimization_barrier(jnp.sum(weights.astype(jnp.float32), axis=-1, keepdims=True))
        return (summed / denominator).astype(jnp.bfloat16)
    heads_out = lax.map(per_head, (split_heads(queries), split_heads(keys_all), split_heads(values_all)))
    attention = jnp.transpose(heads_out, (1, 0, 2)).reshape(tokens_all, HEADS * HEAD)
    updated = hidden.astype(jnp.float32) + modifiers[:, 6] * attention.astype(jnp.float32)
    return updated.astype(jnp.bfloat16)

def reference(state, modulation, noise_level, frame_mask, offset):
    outputs = [section(state[segment_num], modulation[segment_num], noise_level, frame_mask) for segment_num in range(N_SEGMENT)]
    wrapped = jnp.roll(outputs[-1], -offset[0] * FRAME_TOK, axis=0)
    return jnp.stack([wrapped] + outputs[:-1])
```

```python
import functools
import math

import jax
import jax.numpy as jnp
from jax import lax
from jax.experimental import pallas as pl
from jax.experimental.pallas import tpu as pltpu
from jax.sharding import PartitionSpec as P

HEAD = 128
FRAME_TOK = 256

epsilon = 1e-06
negative = -1e30
score_scale = math.log2(math.e) / math.sqrt(HEAD)


def kernel(
    devices,
    segments,
    heads,
    frames,
    rows,
    level_hbm,
    mask_hbm,
    offset_hbm,
    state_ref,
    mod_ref,
    out_ref,
    level_ref,
    mask_ref,
    offset_ref,
    local,
    gathered,
    scale_out,
    scales,
    mods,
    keys,
    values,
    done,
    outgoing,
    scalar_sem,
    local_sem,
    mod_sem,
    state_send,
    state_recv,
    scale_send,
    scale_recv,
    out_send,
    out_recv,
):
    me = lax.axis_index("frame")
    segment = lax.axis_index("segment")
    span = FRAME_TOK // rows
    width = heads * HEAD
    def owner_of(head):
        return head

    my_frame = lax.div(me, span)
    my_part = lax.rem(me, span)
    my_head = lax.min(me, heads - 1)
    owner = me < heads
    my_columns = pl.multiple_of(my_head * HEAD, HEAD)
    my_row = pl.multiple_of(my_part * rows, rows)

    nxt = lax.rem(segment + 1, segments)
    barrier = pltpu.get_barrier_semaphore()

    def greet(peer, peer_segment):
        pl.semaphore_signal(
            barrier,
            inc=1,
            device_id={"frame": peer, "segment": peer_segment},
            device_id_type=pl.DeviceIdType.MESH,
        )

    def greet_reader(index, carry):
        greet(index + jnp.where(index >= me, 1, 0), segment)
        return carry

    def greet_writer(head, carry):
        greet(owner_of(head), lax.rem(segment + segments - 1, segments))
        return carry

    fetch = pltpu.make_async_copy(state_ref.at[0], local, local_sem)
    fetch.start()

    @pl.when(owner)
    def _():
        lax.fori_loop(0, devices - 1, greet_reader, 0)

    if segments > 1:
        lax.fori_loop(0, heads, greet_writer, 0)

    scalar_copies = [
        pltpu.make_async_copy(source, place, scalar_sem.at[index])
        for index, (source, place) in enumerate(
            ((level_hbm, level_ref), (mask_hbm, mask_ref), (offset_hbm, offset_ref))
        )
    ]
    mod_copy = pltpu.make_async_copy(
        mod_ref.at[0, :, :, pl.ds(my_columns, HEAD)], mods, mod_sem
    )

    @pl.when(owner)
    def _():
        mod_copy.start()
        for copy in scalar_copies:
            copy.start()

    fetch.wait()
    widened = local[...].astype(jnp.float32)
    square_mean = jnp.sum(widened * widened, axis=-1, keepdims=True) * (1.0 / width)
    factor = lax.rsqrt(square_mean + epsilon)
    diagonal = lax.broadcasted_iota(jnp.int32, (rows, HEAD), 0) == lax.broadcasted_iota(
        jnp.int32, (rows, HEAD), 1
    )
    scale_out[...] = jnp.sum(
        jnp.where(diagonal, factor, 0.0), axis=0, keepdims=True
    )

    greetings = heads - jnp.where(owner, 1, 0)
    if segments > 1:
        greetings += jnp.where(owner, devices, 0)
    pl.semaphore_wait(barrier, greetings)

    def state_copy(head):
        columns = pl.ds(pl.multiple_of(head * HEAD, HEAD), HEAD)
        return pltpu.make_async_remote_copy(
            src_ref=local.at[:, columns],
            dst_ref=gathered.at[my_frame, pl.ds(my_row, rows), :],
            send_sem=state_send.at[head],
            recv_sem=state_recv.at[my_frame],
            device_id={"frame": owner_of(head)},
            device_id_type=pl.DeviceIdType.MESH,
        )

    def scale_copy(head):
        return pltpu.make_async_remote_copy(
            src_ref=scale_out,
            dst_ref=scales.at[me],
            send_sem=scale_send.at[head],
            recv_sem=scale_recv.at[my_frame],
            device_id={"frame": owner_of(head)},
            device_id_type=pl.DeviceIdType.MESH,
        )

    def for_heads(act):
        part = heads // 2
        begin = lax.rem(lax.div(me, 2) + 0, part)

        for turn in range(2):
            def step(index, carry):
                place = begin + index
                head = 2 * jnp.where(place >= part, place - part, place) + turn

                @pl.when(owner_of(head) != me)
                def _():
                    act(head)

                return carry

            lax.fori_loop(0, part, step, 0)

    def send_rows(head):
        state_copy(head).start()
        scale_copy(head).start()

    def end_rows(head):
        state_copy(head).wait_send()
        scale_copy(head).wait_send()

    for_heads(send_rows)

    @pl.when(owner)
    def _():
        pltpu.make_async_copy(
            local.at[:, pl.ds(my_columns, HEAD)],
            gathered.at[my_frame, pl.ds(my_row, rows), :],
            state_recv.at[my_frame],
        ).start()
        pltpu.make_async_copy(scale_out, scales.at[me], scale_recv.at[my_frame]).start()

    def out_copy(place, part):
        target = place * span + part
        return target, pltpu.make_async_remote_copy(
            src_ref=outgoing.at[place, pl.ds(pl.multiple_of(part * rows, rows), rows), :],
            dst_ref=out_ref.at[0, :, pl.ds(my_columns, HEAD)],
            send_sem=out_send.at[target],
            recv_sem=out_recv,
            device_id={"frame": target, "segment": nxt},
            device_id_type=pl.DeviceIdType.MESH,
        )

    def send_part(place, part, begin):
        target, copy = out_copy(place, part)
        remote = jnp.logical_or(target != me, nxt != segment)

        @pl.when(remote)
        def _():
            if begin:
                copy.start()
            else:
                copy.wait_send()

        if begin:
            @pl.when(jnp.logical_not(remote))
            def _():
                pltpu.make_async_copy(
                    outgoing.at[place, pl.ds(pl.multiple_of(part * rows, rows), rows), :],
                    out_ref.at[0, :, pl.ds(my_columns, HEAD)],
                    out_recv,
                ).start()

    def send_place(place, begin):
        def step(part, carry):
            send_part(place, part, begin)
            return carry

        lax.fori_loop(0, span, step, 0)

    def mod_row(frame, kind):
        return mods[kind, pl.ds(level_ref[frame], 1), :]

    def project(frame):
        query_scale = (1.0 + mod_row(frame, 0)) * score_scale
        query_shift = mod_row(frame, 1) * score_scale
        key_scale, key_shift = 1.0 + mod_row(frame, 2), mod_row(frame, 3)
        value_scale, value_shift = 1.0 + mod_row(frame, 4), mod_row(frame, 5)
        queries = []
        for part in range(span):
            column = jnp.sum(
                jnp.where(diagonal, scales[frame * span + part], 0.0), axis=1, keepdims=True
            )
            inner = slice(part * rows, (part + 1) * rows)
            outer = slice(frame * FRAME_TOK + part * rows, frame * FRAME_TOK + (part + 1) * rows)
            wide = (
                (gathered[frame, inner, :].astype(jnp.float32) * column)
                .astype(jnp.bfloat16)
                .astype(jnp.float32)
            )
            keys[outer, :] = (wide * key_scale + key_shift).astype(jnp.bfloat16)
            values[outer, :] = (wide * value_scale + value_shift).astype(jnp.bfloat16)
            queries.append((wide * query_scale + query_shift).astype(jnp.bfloat16))
        return jnp.concatenate(queries, axis=0)

    def attend(frame, queries):
        def tokens_of(other):
            return slice(other * FRAME_TOK, (other + 1) * FRAME_TOK)

        scores = [
            lax.dot_general(
                queries,
                keys[tokens_of(other), :],
                (((1,), (1,)), ((), ())),
                preferred_element_type=jnp.float32,
            )
            for other in range(frame + 1)
        ]
        top = jnp.max(scores[frame], axis=-1, keepdims=True)
        for other in range(frame):
            peak = jnp.max(scores[other], axis=-1, keepdims=True)
            top = jnp.maximum(top, jnp.where(mask_ref[frame, other] == 1, peak, negative))
        summed, total = 0.0, 0.0
        for other in range(frame + 1):
            floor = top
            if other < frame:
                floor = top + jnp.where(mask_ref[frame, other] == 1, 0.0, -negative)
            weights = jnp.exp2(scores[other] - floor).astype(jnp.bfloat16)
            total += jnp.sum(weights.astype(jnp.float32), axis=-1, keepdims=True)
            summed += jnp.dot(
                weights, values[tokens_of(other), :], preferred_element_type=jnp.float32
            )
        attention = (summed / total).astype(jnp.bfloat16)
        done[frame] = (
            gathered[frame].astype(jnp.float32)
            + mod_row(frame, 6) * attention.astype(jnp.float32)
        ).astype(jnp.bfloat16)

    @pl.when(owner)
    def _():
        mod_copy.wait()
        for copy in scalar_copies:
            copy.wait()
        for batch in [[f] for f in range(frames)]:
            for frame in batch:
                pltpu.make_async_copy(
                    gathered.at[frame], gathered.at[frame], state_recv.at[frame]
                ).wait()
                arrived = scales.at[pl.ds(frame * span, span)]
                pltpu.make_async_copy(arrived, arrived, scale_recv.at[frame]).wait()
            held = [project(frame) for frame in batch]
            for frame, queries in zip(batch, held):
                attend(frame, queries)

        shift = jnp.where(segment == segments - 1, offset_ref[0], 0)
        for place in range(frames):
            outgoing[place] = done[lax.rem(place + shift, frames)]

        def send_all(index, carry):
            part = lax.rem(index + 0, span)
            for place in (3, 2, 1, 0):
                send_part(place, part, True)
            return carry

        lax.fori_loop(0, span, send_all, 0)

    for_heads(end_rows)

    @pl.when(owner)
    def _():
        for place in range(frames):
            send_place(place, False)

    pltpu.make_async_copy(out_ref, out_ref, out_recv).wait()


def body(state, modulation, noise_level, frame_mask, offset):
    _, rows, width = state.shape
    _, levels, kinds, _ = modulation.shape
    devices = lax.axis_size("frame")
    segments = lax.axis_size("segment")
    heads = width // HEAD
    frames = devices * rows // FRAME_TOK
    tokens = devices * rows
    hbm = pl.BlockSpec(memory_space=pl.ANY)
    return pl.pallas_call(
        functools.partial(kernel, devices, segments, heads, frames, rows),
        out_shape=pltpu.VMEM(state.shape, jnp.bfloat16),
        in_specs=[hbm] * 5,
        out_specs=pl.BlockSpec(memory_space=pltpu.VMEM),
        scratch_shapes=[
            pltpu.SMEM(noise_level.shape, jnp.int32),
            pltpu.SMEM(frame_mask.shape, jnp.int32),
            pltpu.SMEM(offset.shape, jnp.int32),
            pltpu.VMEM((rows, width), jnp.bfloat16),
            pltpu.VMEM((frames, FRAME_TOK, HEAD), jnp.bfloat16),
            pltpu.VMEM((1, HEAD), jnp.float32),
            pltpu.VMEM((devices, 1, HEAD), jnp.float32),
            pltpu.VMEM((kinds, levels, HEAD), jnp.float32),
            pltpu.VMEM((tokens, HEAD), jnp.bfloat16),
            pltpu.VMEM((tokens, HEAD), jnp.bfloat16),
            pltpu.VMEM((frames, FRAME_TOK, HEAD), jnp.bfloat16),
            pltpu.VMEM((frames, FRAME_TOK, HEAD), jnp.bfloat16),
            pltpu.SemaphoreType.DMA((3,)),
            pltpu.SemaphoreType.DMA,
            pltpu.SemaphoreType.DMA,
            pltpu.SemaphoreType.DMA((heads,)),
            pltpu.SemaphoreType.DMA((frames,)),
            pltpu.SemaphoreType.DMA((heads,)),
            pltpu.SemaphoreType.DMA((frames,)),
            pltpu.SemaphoreType.DMA((devices,)),
            pltpu.SemaphoreType.DMA,
        ],
        compiler_params=pltpu.CompilerParams(has_side_effects=True, collective_id=0),
        name="denoise",
    )(noise_level, frame_mask, offset, state, jnp.swapaxes(modulation, 1, 2))


def solution(mesh):
    return jax.shard_map(
        body,
        mesh=mesh,
        in_specs=(P("segment", "frame", None), P("segment", None, None, None), P(), P(), P()),
        out_specs=P("segment", "frame", None),
        check_vma=False,
    )
```

```python
import functools
import math

import jax
import jax.numpy as jnp
from jax import lax
from jax.experimental import pallas as pl
from jax.experimental.pallas import tpu as pltpu
from jax.sharding import PartitionSpec as P

HEAD = 128
FRAME_TOK = 256

epsilon = 1e-06
negative = -1e30
score_scale = math.log2(math.e) / math.sqrt(HEAD)


def owner_rounds(heads, span):
    if heads % span or span % 2:
        return [(0, 1, heads)]
    groups = heads // span
    evens = [(group * span, 2, span // 2) for group in [*range(1, groups), 0]]
    return evens + [(first + 1, 2, count) for first, _, count in reversed(evens)]


def kernel(
    devices,
    segments,
    heads,
    frames,
    rows,
    level_hbm,
    mask_hbm,
    offset_hbm,
    state_ref,
    mod_ref,
    out_ref,
    level_ref,
    mask_ref,
    offset_ref,
    local,
    gathered,
    scale_out,
    scales,
    mods,
    keys,
    values,
    done,
    outgoing,
    scalar_sem,
    local_sem,
    mod_sem,
    state_send,
    state_recv,
    scale_send,
    scale_recv,
    out_send,
    out_recv,
):
    me = lax.axis_index("frame")
    segment = lax.axis_index("segment")
    span = FRAME_TOK // rows
    width = heads * HEAD
    plan = owner_rounds(heads, span)
    my_frame = lax.div(me, span)
    my_part = lax.rem(me, span)
    my_row = pl.multiple_of(my_part * rows, rows)

    owner, my_head, base = me < 0, 0, 0
    rounds = []
    for first, stride, count in plan:
        rounds.append((base, first, stride, count))
        place = me - first
        inside = jnp.logical_and(place >= 0, place < stride * count)
        if stride > 1:
            inside = jnp.logical_and(inside, lax.rem(place + stride * devices, stride) == 0)
        owner = jnp.logical_or(owner, inside)
        my_head = jnp.where(inside, base + lax.div(place, stride), my_head)
        if base == 0:
            early = inside
        base += count

    nxt = lax.rem(segment + 1, segments)
    barrier = pltpu.get_barrier_semaphore()

    def columns_of(head):
        return pl.ds(pl.multiple_of(head * HEAD, HEAD), HEAD)

    def greet(peer, peer_segment):
        pl.semaphore_signal(
            barrier,
            inc=1,
            device_id={"frame": peer, "segment": peer_segment},
            device_id_type=pl.DeviceIdType.MESH,
        )

    def greet_reader(index, carry):
        greet(index + jnp.where(index >= me, 1, 0), segment)
        return carry

    fetches = [
        pltpu.make_async_copy(
            state_ref.at[0, :, pl.ds(piece * (width // 1), width // 1)],
            local.at[:, pl.ds(piece * (width // 1), width // 1)],
            local_sem.at[piece],
        )
        for piece in range(1)
    ]
    for fetch in fetches:
        fetch.start()

    @pl.when(owner)
    def _():
        lax.fori_loop(0, devices - 1, greet_reader, 0)

    if segments > 1:
        for _, first, stride, count in rounds:

            def greet_writer(index, carry):
                greet(first + stride * index, lax.rem(segment + segments - 1, segments))
                return carry

            lax.fori_loop(0, count, greet_writer, 0)

    scalar_copies = [
        pltpu.make_async_copy(source, place, scalar_sem.at[index])
        for index, (source, place) in enumerate(
            ((level_hbm, level_ref), (mask_hbm, mask_ref), (offset_hbm, offset_ref))
        )
    ]
    mod_copy = pltpu.make_async_copy(
        mod_ref.at[0, :, :, columns_of(my_head)], mods, mod_sem
    )

    @pl.when(owner)
    def _():
        mod_copy.start()
        for copy in scalar_copies:
            copy.start()

    for fetch in fetches:
        fetch.wait()
    widened = local[...].astype(jnp.float32)
    square_mean = jnp.sum(widened * widened, axis=-1, keepdims=True) * (1.0 / width)
    factor = lax.rsqrt(square_mean + epsilon)
    diagonal = lax.broadcasted_iota(jnp.int32, (rows, HEAD), 0) == lax.broadcasted_iota(
        jnp.int32, (rows, HEAD), 1
    )
    scale_out[...] = jnp.sum(
        jnp.where(diagonal, factor, 0.0), axis=0, keepdims=True
    )

    greetings = heads - jnp.where(owner, 1, 0)
    if segments > 1:
        greetings += jnp.where(owner, devices, 0)
    pl.semaphore_wait(barrier, greetings)

    def copies_to(head, peer):
        return (
            pltpu.make_async_remote_copy(
                src_ref=local.at[:, columns_of(head)],
                dst_ref=gathered.at[my_frame, pl.ds(my_row, rows), :],
                send_sem=state_send.at[head],
                recv_sem=state_recv.at[my_frame],
                device_id={"frame": peer},
                device_id_type=pl.DeviceIdType.MESH,
            ),
            pltpu.make_async_remote_copy(
                src_ref=scale_out,
                dst_ref=scales.at[me],
                send_sem=scale_send.at[head],
                recv_sem=scale_recv.at[my_frame],
                device_id={"frame": peer},
                device_id_type=pl.DeviceIdType.MESH,
            ),
        )

    def for_heads(act):
        for base, first, stride, count in rounds:
            turn = lax.rem(lax.div(me, 2) + 1, count)

            def each(index, carry):
                index += turn
                index = jnp.where(index >= count, index - count, index)
                peer = first + stride * index

                @pl.when(peer != me)
                def _():
                    for copy in copies_to(base + index, peer):
                        act(copy)

                return carry

            lax.fori_loop(0, count, each, 0)

    for_heads(lambda copy: copy.start())

    @pl.when(owner)
    def _():
        pltpu.make_async_copy(
            local.at[:, columns_of(my_head)],
            gathered.at[my_frame, pl.ds(my_row, rows), :],
            state_recv.at[my_frame],
        ).start()
        pltpu.make_async_copy(scale_out, scales.at[me], scale_recv.at[my_frame]).start()

    def send_part(place, part, begin):
        target = place * span + part
        source = outgoing.at[place, pl.ds(pl.multiple_of(part * rows, rows), rows), :]
        goal = out_ref.at[0, :, columns_of(my_head)]
        copy = pltpu.make_async_remote_copy(
            src_ref=source,
            dst_ref=goal,
            send_sem=out_send.at[target],
            recv_sem=out_recv,
            device_id={"frame": target, "segment": nxt},
            device_id_type=pl.DeviceIdType.MESH,
        )
        remote = jnp.logical_or(target != me, nxt != segment)

        @pl.when(remote)
        def _():
            if begin:
                copy.start()
            else:
                copy.wait_send()

        if begin:
            @pl.when(jnp.logical_not(remote))
            def _():
                pltpu.make_async_copy(source, goal, out_recv).start()

    def send_all(begin):
        def each(index, carry):
            part = lax.rem(index + 0, span)
            for turn in range(frames):
                place = jnp.where(2 * me >= devices, turn, frames - 1 - turn)
                send_part(place, part, begin)
            return carry

        lax.fori_loop(0, span, each, 0)

    def tokens_of(frame):
        return slice(frame * FRAME_TOK, (frame + 1) * FRAME_TOK)

    def mod_row(frame, kind):
        return mods[kind, pl.ds(level_ref[frame], 1), :]

    def project(frame):
        query_scale = (1.0 + mod_row(frame, 0)) * score_scale
        query_shift = mod_row(frame, 1) * score_scale
        key_scale, key_shift = 1.0 + mod_row(frame, 2), mod_row(frame, 3)
        value_scale, value_shift = 1.0 + mod_row(frame, 4), mod_row(frame, 5)
        queries = []
        for part in range(span):
            column = jnp.sum(
                jnp.where(diagonal, scales[frame * span + part], 0.0), axis=1, keepdims=True
            )
            inner = slice(part * rows, (part + 1) * rows)
            outer = slice(frame * FRAME_TOK + part * rows, frame * FRAME_TOK + (part + 1) * rows)
            wide = (
                (gathered[frame, inner, :].astype(jnp.float32) * column)
                .astype(jnp.bfloat16)
                .astype(jnp.float32)
            )
            keys[outer, :] = (wide * key_scale + key_shift).astype(jnp.bfloat16)
            values[outer, :] = (wide * value_scale + value_shift).astype(jnp.bfloat16)
            queries.append((wide * query_scale + query_shift).astype(jnp.bfloat16))
        return jnp.concatenate(queries, axis=0)

    def attend(frame, queries):
        scores = [
            lax.dot_general(
                queries,
                keys[tokens_of(other), :],
                (((1,), (1,)), ((), ())),
                preferred_element_type=jnp.float32,
            )
            for other in range(frame + 1)
        ]
        top = jnp.max(scores[frame], axis=-1, keepdims=True)
        for other in range(frame):
            peak = jnp.max(scores[other], axis=-1, keepdims=True)
            top = jnp.maximum(top, jnp.where(mask_ref[frame, other] == 1, peak, negative))
        summed, total = 0.0, 0.0
        for other in range(frame + 1):
            floor = top
            if other < frame:
                floor = top + jnp.where(mask_ref[frame, other] == 1, 0.0, -negative)
            weights = jnp.exp2(scores[other] - floor).astype(jnp.bfloat16)
            total += jnp.sum(weights.astype(jnp.float32), axis=-1, keepdims=True)
            summed += jnp.dot(
                weights, values[tokens_of(other), :], preferred_element_type=jnp.float32
            )
        attention = (summed / total).astype(jnp.bfloat16)
        done[frame] = (
            gathered[frame].astype(jnp.float32)
            + mod_row(frame, 6) * attention.astype(jnp.float32)
        ).astype(jnp.bfloat16)

    def in_order(batches):
        for batch in batches:
            for frame in batch:
                pltpu.make_async_copy(
                    gathered.at[frame], gathered.at[frame], state_recv.at[frame]
                ).wait()
                arrived = scales.at[pl.ds(frame * span, span)]
                pltpu.make_async_copy(arrived, arrived, scale_recv.at[frame]).wait()
            held = [project(frame) for frame in batch]
            for frame, queries in zip(batch, held):
                attend(frame, queries)

    @pl.when(owner)
    def _():
        mod_copy.wait()
        for copy in scalar_copies:
            copy.wait()
        @pl.when(jnp.logical_or(2 * me >= devices, early))
        def _():
            in_order([list(range(frames))])

        @pl.when(jnp.logical_not(jnp.logical_or(2 * me >= devices, early)))
        def _():
            in_order([[f] for f in range(frames - 2)] + [[frames - 2, frames - 1]])

        shift = jnp.where(segment == segments - 1, offset_ref[0], 0)
        for place in range(frames):
            outgoing[place] = done[lax.rem(place + shift, frames)]
        send_all(True)

    for_heads(lambda copy: copy.wait_send())

    @pl.when(owner)
    def _():
        send_all(False)

    pltpu.make_async_copy(out_ref, out_ref, out_recv).wait()


def body(state, modulation, noise_level, frame_mask, offset):
    _, rows, width = state.shape
    _, levels, kinds, _ = modulation.shape
    devices = lax.axis_size("frame")
    segments = lax.axis_size("segment")
    heads = width // HEAD
    frames = devices * rows // FRAME_TOK
    tokens = devices * rows
    hbm = pl.BlockSpec(memory_space=pl.ANY)
    return pl.pallas_call(
        functools.partial(kernel, devices, segments, heads, frames, rows),
        out_shape=pltpu.VMEM(state.shape, jnp.bfloat16),
        in_specs=[hbm] * 5,
        out_specs=pl.BlockSpec(memory_space=pltpu.VMEM),
        scratch_shapes=[
            pltpu.SMEM(noise_level.shape, jnp.int32),
            pltpu.SMEM(frame_mask.shape, jnp.int32),
            pltpu.SMEM(offset.shape, jnp.int32),
            pltpu.VMEM((rows, width), jnp.bfloat16),
            pltpu.VMEM((frames, FRAME_TOK, HEAD), jnp.bfloat16),
            pltpu.VMEM((1, HEAD), jnp.float32),
            pltpu.VMEM((devices, 1, HEAD), jnp.float32),
            pltpu.VMEM((kinds, levels, HEAD), jnp.float32),
            pltpu.VMEM((tokens, HEAD), jnp.bfloat16),
            pltpu.VMEM((tokens, HEAD), jnp.bfloat16),
            pltpu.VMEM((frames, FRAME_TOK, HEAD), jnp.bfloat16),
            pltpu.VMEM((frames, FRAME_TOK, HEAD), jnp.bfloat16),
            pltpu.SemaphoreType.DMA((3,)),
            pltpu.SemaphoreType.DMA((1,)),
            pltpu.SemaphoreType.DMA,
            pltpu.SemaphoreType.DMA((heads,)),
            pltpu.SemaphoreType.DMA((frames,)),
            pltpu.SemaphoreType.DMA((heads,)),
            pltpu.SemaphoreType.DMA((frames,)),
            pltpu.SemaphoreType.DMA((devices,)),
            pltpu.SemaphoreType.DMA,
        ],
        compiler_params=pltpu.CompilerParams(has_side_effects=True, collective_id=0),
        name="denoise",
    )(noise_level, frame_mask, offset, state, jnp.swapaxes(modulation, 1, 2))


def solution(mesh):
    return jax.shard_map(
        body,
        mesh=mesh,
        in_specs=(P("segment", "frame", None), P("segment", None, None, None), P(), P(), P()),
        out_specs=P("segment", "frame", None),
        check_vma=False,
    )
```

```python
import functools
import math

import jax
import jax.numpy as jnp
from jax import lax
from jax.experimental import pallas as pl
from jax.experimental.pallas import tpu as pltpu
from jax.sharding import PartitionSpec as P

HEAD = 128
FRAME_TOK = 256

epsilon = 1e-06
negative = -1e30
score_scale = math.log2(math.e) / math.sqrt(HEAD)


def owner_rounds(heads, span):
    if heads % span or span % 2:
        return [(0, 1, heads)]
    groups = heads // span
    evens = [(group * span, 2, span // 2) for group in [*range(1, groups), 0]]
    return evens + [(first + 1, 2, count) for first, _, count in reversed(evens)]


def kernel(
    devices,
    segments,
    heads,
    frames,
    rows,
    level_hbm,
    mask_hbm,
    offset_hbm,
    state_ref,
    mod_ref,
    out_ref,
    level_ref,
    mask_ref,
    offset_ref,
    local,
    gathered,
    scale_out,
    scales,
    mods,
    keys,
    values,
    done,
    outgoing,
    scalar_sem,
    local_sem,
    mod_sem,
    state_send,
    state_recv,
    scale_send,
    scale_recv,
    out_send,
    out_recv,
    late_sem,
):
    me = lax.axis_index("frame")
    segment = lax.axis_index("segment")
    span = FRAME_TOK // rows
    width = heads * HEAD
    plan = owner_rounds(heads, span)
    shared = heads % span == 0 and heads // span + 1 == frames
    last = devices - span
    my_frame = lax.div(me, span)
    my_part = lax.rem(me, span)
    my_row = pl.multiple_of(my_part * rows, rows)

    owner, my_head, base = me < 0, 0, 0
    rounds = []
    for first, stride, count in plan:
        rounds.append((base, first, stride, count))
        place = me - first
        inside = jnp.logical_and(place >= 0, place < stride * count)
        if stride > 1:
            inside = jnp.logical_and(inside, lax.rem(place + stride * devices, stride) == 0)
        owner = jnp.logical_or(owner, inside)
        my_head = jnp.where(inside, base + lax.div(place, stride), my_head)
        if base == 0:
            early = inside
        base += count

    leader = owner
    late = me >= last
    split = frames - 1
    low, high = 0, frames
    if shared:
        for base, first, stride, count in list(rounds):
            if first < span:
                rounds.append((base, first + last, stride, count))
                place = me - last - first
                inside = jnp.logical_and(place >= 0, lax.rem(place + stride * devices, stride) == 0)
                my_head = jnp.where(inside, base + lax.div(place, stride), my_head)
        owner = jnp.logical_or(owner, late)
        low = jnp.where(late, split, 0)
        high = jnp.where(me < span, split, frames)

    nxt = lax.rem(segment + 1, segments)
    barrier = pltpu.get_barrier_semaphore()

    def columns_of(head):
        return pl.ds(pl.multiple_of(head * HEAD, HEAD), HEAD)

    def greet(peer, peer_segment):
        pl.semaphore_signal(
            barrier,
            inc=1,
            device_id={"frame": peer, "segment": peer_segment},
            device_id_type=pl.DeviceIdType.MESH,
        )

    def greet_reader(index, carry):
        greet(index + jnp.where(index >= me, 1, 0), segment)
        return carry

    fetches = [
        pltpu.make_async_copy(
            state_ref.at[0, :, pl.ds(piece * (width // 1), width // 1)],
            local.at[:, pl.ds(piece * (width // 1), width // 1)],
            local_sem.at[piece],
        )
        for piece in range(1)
    ]
    for fetch in fetches:
        fetch.start()

    @pl.when(leader)
    def _():
        lax.fori_loop(0, devices - 1, greet_reader, 0)

    if shared:
        @pl.when(late)
        def _():
            lax.fori_loop(last, devices - 1, greet_reader, 0)

    if segments > 1:
        for _, first, stride, count in rounds:

            def greet_writer(index, carry):
                greet(first + stride * index, lax.rem(segment + segments - 1, segments))
                return carry

            lax.fori_loop(0, count, greet_writer, 0)

    scalar_copies = [
        pltpu.make_async_copy(source, place, scalar_sem.at[index])
        for index, (source, place) in enumerate(
            ((level_hbm, level_ref), (mask_hbm, mask_ref), (offset_hbm, offset_ref))
        )
    ]
    mod_copy = pltpu.make_async_copy(
        mod_ref.at[0, :, :, columns_of(my_head)], mods, mod_sem
    )

    @pl.when(owner)
    def _():
        mod_copy.start()
        for copy in scalar_copies:
            copy.start()

    for fetch in fetches:
        fetch.wait()
    widened = local[...].astype(jnp.float32)
    square_mean = jnp.sum(widened * widened, axis=-1, keepdims=True) * (1.0 / width)
    factor = lax.rsqrt(square_mean + epsilon)
    diagonal = lax.broadcasted_iota(jnp.int32, (rows, HEAD), 0) == lax.broadcasted_iota(
        jnp.int32, (rows, HEAD), 1
    )
    scale_out[...] = jnp.sum(
        jnp.where(diagonal, factor, 0.0), axis=0, keepdims=True
    )

    greetings = heads - jnp.where(leader, 1, 0)
    if shared:
        greetings += jnp.where(late, span - 1, 0)
    if segments > 1:
        greetings += jnp.where(owner, devices, 0)
    pl.semaphore_wait(barrier, greetings)

    def copies_to(head, peer):
        return (
            pltpu.make_async_remote_copy(
                src_ref=local.at[:, columns_of(head)],
                dst_ref=gathered.at[my_frame, pl.ds(my_row, rows), :],
                send_sem=state_send,
                recv_sem=state_recv.at[my_frame],
                device_id={"frame": peer},
                device_id_type=pl.DeviceIdType.MESH,
            ),
            pltpu.make_async_remote_copy(
                src_ref=scale_out,
                dst_ref=scales.at[me],
                send_sem=scale_send,
                recv_sem=scale_recv.at[my_frame],
                device_id={"frame": peer},
                device_id_type=pl.DeviceIdType.MESH,
            ),
        )

    def for_heads(chosen, act):
        for base, first, stride, count in chosen:
            turn = lax.rem(lax.div(me, 2) + 1, count)

            def each(index, carry):
                index += turn
                index = jnp.where(index >= count, index - count, index)
                peer = first + stride * index

                @pl.when(peer != me)
                def _():
                    for copy in copies_to(base + index, peer):
                        act(copy)

                return carry

            lax.fori_loop(0, count, each, 0)

    for_heads(rounds[: len(plan)], lambda copy: copy.start())

    if shared:
        def admit(peer, carry):
            pl.semaphore_signal(
                late_sem,
                inc=1,
                device_id={"frame": peer},
                device_id_type=pl.DeviceIdType.MESH,
            )
            return carry

        @pl.when(late)
        def _():
            lax.fori_loop(0, last, admit, 0)

        @pl.when(jnp.logical_not(late))
        def _():
            pl.semaphore_wait(late_sem, span)

        for_heads(rounds[len(plan) :], lambda copy: copy.start())

    @pl.when(owner)
    def _():
        pltpu.make_async_copy(
            local.at[:, columns_of(my_head)],
            gathered.at[my_frame, pl.ds(my_row, rows), :],
            state_recv.at[my_frame],
        ).start()
        pltpu.make_async_copy(scale_out, scales.at[me], scale_recv.at[my_frame]).start()

    def send_part(place, part):
        target = place * span + part
        source = outgoing.at[place, pl.ds(pl.multiple_of(part * rows, rows), rows), :]
        goal = out_ref.at[0, :, columns_of(my_head)]
        remote = jnp.logical_or(target != me, nxt != segment)

        @pl.when(remote)
        def _():
            pltpu.make_async_remote_copy(
                src_ref=source,
                dst_ref=goal,
                send_sem=out_send,
                recv_sem=out_recv,
                device_id={"frame": target, "segment": nxt},
                device_id_type=pl.DeviceIdType.MESH,
            ).start()

        @pl.when(jnp.logical_not(remote))
        def _():
            pltpu.make_async_copy(source, goal, out_recv).start()

    def send_all():
        def each(index, carry):
            part = index

            def one(turn, carry):
                place = jnp.where(2 * me >= devices, low + turn, high - 1 - turn)
                send_part(place, part)
                return carry

            return lax.fori_loop(0, high - low, one, carry)

        lax.fori_loop(0, span, each, 0)


    def sent(count, send_sem):
        pieces = keys.at[pl.ds(0, count * rows), :]
        pltpu.make_async_copy(pieces, pieces, send_sem).wait()

    def sent_rows(count):
        sent(count, state_send)
        factors = scales.at[pl.ds(0, count)]
        pltpu.make_async_copy(factors, factors, scale_send).wait()

    def tokens_of(frame):
        return slice(frame * FRAME_TOK, (frame + 1) * FRAME_TOK)

    def mod_row(frame, kind):
        return mods[kind, pl.ds(level_ref[frame], 1), :]

    def project(frame):
        query_scale = (1.0 + mod_row(frame, 0)) * score_scale
        query_shift = mod_row(frame, 1) * score_scale
        key_scale, key_shift = 1.0 + mod_row(frame, 2), mod_row(frame, 3)
        value_scale, value_shift = 1.0 + mod_row(frame, 4), mod_row(frame, 5)
        queries = []
        for part in range(span):
            column = jnp.sum(
                jnp.where(diagonal, scales[frame * span + part], 0.0), axis=1, keepdims=True
            )
            inner = slice(part * rows, (part + 1) * rows)
            outer = slice(frame * FRAME_TOK + part * rows, frame * FRAME_TOK + (part + 1) * rows)
            wide = (
                (gathered[frame, inner, :].astype(jnp.float32) * column)
                .astype(jnp.bfloat16)
                .astype(jnp.float32)
            )
            keys[outer, :] = (wide * key_scale + key_shift).astype(jnp.bfloat16)
            values[outer, :] = (wide * value_scale + value_shift).astype(jnp.bfloat16)
            queries.append((wide * query_scale + query_shift).astype(jnp.bfloat16))
        return jnp.concatenate(queries, axis=0)

    def attend(frame, queries):
        scores = [
            lax.dot_general(
                queries,
                keys[tokens_of(other), :],
                (((1,), (1,)), ((), ())),
                preferred_element_type=jnp.float32,
            )
            for other in range(frame + 1)
        ]
        top = jnp.max(scores[frame], axis=-1, keepdims=True)
        for other in range(frame):
            peak = jnp.max(scores[other], axis=-1, keepdims=True)
            top = jnp.maximum(top, jnp.where(mask_ref[frame, other] == 1, peak, negative))
        summed, total = 0.0, 0.0
        for other in range(frame + 1):
            floor = top
            if other < frame:
                floor = top + jnp.where(mask_ref[frame, other] == 1, 0.0, -negative)
            weights = jnp.exp2(scores[other] - floor).astype(jnp.bfloat16)
            total += jnp.sum(weights.astype(jnp.float32), axis=-1, keepdims=True)
            summed += jnp.dot(
                weights, values[tokens_of(other), :], preferred_element_type=jnp.float32
            )
        attention = (summed / total).astype(jnp.bfloat16)
        done[frame] = (
            gathered[frame].astype(jnp.float32)
            + mod_row(frame, 6) * attention.astype(jnp.float32)
        ).astype(jnp.bfloat16)

    def in_order(batches):
        for batch in batches:
            for frame in batch:
                pltpu.make_async_copy(
                    gathered.at[frame], gathered.at[frame], state_recv.at[frame]
                ).wait()
                arrived = scales.at[pl.ds(frame * span, span)]
                pltpu.make_async_copy(arrived, arrived, scale_recv.at[frame]).wait()
            held = [project(frame) for frame in batch]
            for frame, queries in zip(batch, held):
                attend(frame, queries)

    @pl.when(owner)
    def _():
        mod_copy.wait()
        for copy in scalar_copies:
            copy.wait()
        @pl.when(jnp.logical_or(2 * me >= devices, early))
        def _():
            in_order([list(range(frames))])

        @pl.when(jnp.logical_not(jnp.logical_or(2 * me >= devices, early)))
        def _():
            in_order([[f] for f in range(frames - 2)] + [[frames - 2, frames - 1]])

        shift = jnp.where(segment == segments - 1, offset_ref[0], 0)
        for place in range(frames):
            outgoing[place] = done[lax.rem(place + shift, frames)]
        send_all()

    kept = 1 if segments == 1 else 0
    if shared:
        sent_rows(heads + span - 1)
        for chosen, count in (
            (me < span, split),
            (late, frames - split),
            (jnp.logical_and(me >= span, me < last), frames),
        ):
            @pl.when(chosen)
            def _():
                sent(count * span - kept, out_send)
    else:
        @pl.when(owner)
        def _():
            sent_rows(heads - 1)
            sent(frames * span - kept, out_send)

        @pl.when(jnp.logical_not(owner))
        def _():
            sent_rows(heads)

    pltpu.make_async_copy(out_ref, out_ref, out_recv).wait()


def body(state, modulation, noise_level, frame_mask, offset):
    _, rows, width = state.shape
    _, levels, kinds, _ = modulation.shape
    devices = lax.axis_size("frame")
    segments = lax.axis_size("segment")
    heads = width // HEAD
    frames = devices * rows // FRAME_TOK
    tokens = devices * rows
    hbm = pl.BlockSpec(memory_space=pl.ANY)
    return pl.pallas_call(
        functools.partial(kernel, devices, segments, heads, frames, rows),
        out_shape=pltpu.VMEM(state.shape, jnp.bfloat16),
        in_specs=[hbm] * 5,
        out_specs=pl.BlockSpec(memory_space=pltpu.VMEM),
        scratch_shapes=[
            pltpu.SMEM(noise_level.shape, jnp.int32),
            pltpu.SMEM(frame_mask.shape, jnp.int32),
            pltpu.SMEM(offset.shape, jnp.int32),
            pltpu.VMEM((rows, width), jnp.bfloat16),
            pltpu.VMEM((frames, FRAME_TOK, HEAD), jnp.bfloat16),
            pltpu.VMEM((1, HEAD), jnp.float32),
            pltpu.VMEM((devices, 1, HEAD), jnp.float32),
            pltpu.VMEM((kinds, levels, HEAD), jnp.float32),
            pltpu.VMEM((tokens, HEAD), jnp.bfloat16),
            pltpu.VMEM((tokens, HEAD), jnp.bfloat16),
            pltpu.VMEM((frames, FRAME_TOK, HEAD), jnp.bfloat16),
            pltpu.VMEM((frames, FRAME_TOK, HEAD), jnp.bfloat16),
            pltpu.SemaphoreType.DMA((3,)),
            pltpu.SemaphoreType.DMA((1,)),
            pltpu.SemaphoreType.DMA,
            pltpu.SemaphoreType.DMA,
            pltpu.SemaphoreType.DMA((frames,)),
            pltpu.SemaphoreType.DMA,
            pltpu.SemaphoreType.DMA((frames,)),
            pltpu.SemaphoreType.DMA,
            pltpu.SemaphoreType.DMA,
            pltpu.SemaphoreType.REGULAR,
        ],
        compiler_params=pltpu.CompilerParams(has_side_effects=True, collective_id=0),
        name="denoise",
    )(noise_level, frame_mask, offset, state, jnp.swapaxes(modulation, 1, 2))


def solution(mesh):
    return jax.shard_map(
        body,
        mesh=mesh,
        in_specs=(P("segment", "frame", None), P("segment", None, None, None), P(), P(), P()),
        out_specs=P("segment", "frame", None),
        check_vma=False,
    )
```

```python
import functools
import math

import jax
import jax.numpy as jnp
from jax import lax
from jax.experimental import pallas as pl
from jax.experimental.pallas import tpu as pltpu
from jax.sharding import PartitionSpec as P

HEAD = 128
FRAME_TOK = 256

LEAD = 2

epsilon = 1e-06
negative = -1e30
score_scale = math.log2(math.e) / math.sqrt(HEAD)


def owner_plan(heads, devices, span):
    groups = heads // span
    if heads % span or span % 4 or (groups + 1) * span != devices or groups < 2:
        return [(0, 1, heads)], [], []
    last = devices - span
    pairs = span // 2
    order = [*range(1, groups), 0]
    evens = [(group * span, 2, pairs) for group in order]
    odds = [(group * span + 1, 2, pairs) for group in reversed(order)]
    return evens + odds, [], [(groups - 1, last, 2, pairs), (groups, last + 1, 2, pairs)]

def kernel(
    devices,
    segments,
    heads,
    frames,
    rows,
    level_hbm,
    mask_hbm,
    offset_hbm,
    state_ref,
    mod_ref,
    out_ref,
    level_ref,
    mask_ref,
    offset_ref,
    local,
    gathered,
    scale_out,
    scales,
    mods,
    keys,
    values,
    done,
    outgoing,
    scalar_sem,
    local_sem,
    mod_sem,
    state_send,
    state_recv,
    scale_send,
    scale_recv,
    out_send,
    out_recv,
    late_sem,
):
    me = lax.axis_index("frame")
    segment = lax.axis_index("segment")
    span = FRAME_TOK // rows
    width = heads * HEAD
    early_plan, late_plan, doubles = owner_plan(heads, devices, span)
    shared = bool(doubles)
    last = devices - span
    my_frame = lax.div(me, span)
    my_part = lax.rem(me, span)
    my_row = pl.multiple_of(my_part * rows, rows)

    def among(first, stride, count):
        place = me - first
        inside = jnp.logical_and(place >= 0, place < stride * count)
        if stride > 1:
            inside = jnp.logical_and(inside, lax.rem(place + stride * devices, stride) == 0)
        return inside, lax.div(place, stride)

    split = frames - 1
    owner, my_head, base, low, high = me < 0, 0, 0, 0, frames
    rounds, late_rounds = [], []
    for index, (first, stride, count) in enumerate(early_plan + late_plan):
        entry = (base, first, stride, count)
        (rounds if index < len(early_plan) else late_rounds).append(entry)
        inside, rank = among(first, stride, count)
        owner = jnp.logical_or(owner, inside)
        my_head = jnp.where(inside, base + rank, my_head)
        if index == 0:
            early = inside
        base += count
    leader, late = owner, me < 0
    lower, upper = me < 0, me < 0
    for index, first, stride, count in doubles:
        base, lower_first, lower_stride, _ = rounds[index]
        late_rounds.append((base, first, stride, count))
        inside, rank = among(first, stride, count)
        owner = jnp.logical_or(owner, inside)
        my_head = jnp.where(inside, base + rank, my_head)
        upper = jnp.logical_or(upper, inside)
        lower = jnp.logical_or(lower, among(lower_first, lower_stride, count)[0])
    if shared:
        late = me >= last
        leader = jnp.logical_not(late)
        low = jnp.where(upper, split, 0)
        high = jnp.where(lower, split, frames)
    copies = sum(entry[3] for entry in rounds + late_rounds)

    second_half = 2 * me >= devices
    far = my_part >= span - span // 4
    nxt = lax.rem(segment + 1, segments)
    barrier = pltpu.get_barrier_semaphore()

    def columns_of(head):
        return pl.ds(pl.multiple_of(head * HEAD, HEAD), HEAD)

    def greet(peer, peer_segment):
        pl.semaphore_signal(
            barrier,
            inc=1,
            device_id={"frame": peer, "segment": peer_segment},
            device_id_type=pl.DeviceIdType.MESH,
        )

    def greet_reader(index, carry):
        greet(index + jnp.where(index >= me, 1, 0), segment)
        return carry

    fetches = [
        pltpu.make_async_copy(
            state_ref.at[0, :, pl.ds(piece * (width // 1), width // 1)],
            local.at[:, pl.ds(piece * (width // 1), width // 1)],
            local_sem.at[piece],
        )
        for piece in range(1)
    ]
    for fetch in fetches:
        fetch.start()

    @pl.when(leader)
    def _():
        lax.fori_loop(0, devices - 1, greet_reader, 0)

    if shared:
        @pl.when(late)
        def _():
            lax.fori_loop(last, devices - 1, greet_reader, 0)

    if segments > 1:
        for _, first, stride, count in rounds + late_rounds:

            def greet_writer(index, carry):
                greet(first + stride * index, lax.rem(segment + segments - 1, segments))
                return carry

            lax.fori_loop(0, count, greet_writer, 0)

    scalar_copies = [
        pltpu.make_async_copy(source, place, scalar_sem.at[index])
        for index, (source, place) in enumerate(
            ((level_hbm, level_ref), (mask_hbm, mask_ref), (offset_hbm, offset_ref))
        )
    ]
    mod_copy = pltpu.make_async_copy(
        mod_ref.at[0, :, :, columns_of(my_head)], mods, mod_sem
    )

    @pl.when(owner)
    def _():
        mod_copy.start()
        for copy in scalar_copies:
            copy.start()

    for fetch in fetches:
        fetch.wait()
    widened = local[...].astype(jnp.float32)
    square_mean = jnp.sum(widened * widened, axis=-1, keepdims=True) * (1.0 / width)
    factor = lax.rsqrt(square_mean + epsilon)
    diagonal = lax.broadcasted_iota(jnp.int32, (rows, HEAD), 0) == lax.broadcasted_iota(
        jnp.int32, (rows, HEAD), 1
    )
    scale_out[...] = jnp.sum(
        jnp.where(diagonal, factor, 0.0), axis=0, keepdims=True
    )

    greetings = (last if shared else heads) - jnp.where(leader, 1, 0)
    if shared:
        greetings += jnp.where(late, span - 1, 0)
    if segments > 1:
        greetings += jnp.where(owner, devices, 0)
    pl.semaphore_wait(barrier, greetings)

    def copies_to(head, peer):
        return (
            pltpu.make_async_remote_copy(
                src_ref=local.at[:, columns_of(head)],
                dst_ref=gathered.at[my_frame, pl.ds(my_row, rows), :],
                send_sem=state_send,
                recv_sem=state_recv.at[my_frame],
                device_id={"frame": peer},
                device_id_type=pl.DeviceIdType.MESH,
            ),
            pltpu.make_async_remote_copy(
                src_ref=scale_out,
                dst_ref=scales.at[me],
                send_sem=scale_send,
                recv_sem=scale_recv.at[my_frame],
                device_id={"frame": peer},
                device_id_type=pl.DeviceIdType.MESH,
            ),
        )

    def for_heads(chosen, act):
        for base, first, stride, count in chosen:
            turn = lax.rem(lax.div(me, 2) + 1, count)

            def each(index, carry):
                index += turn
                index = jnp.where(index >= count, index - count, index)
                peer = first + stride * index

                @pl.when(peer != me)
                def _():
                    for copy in copies_to(base + index, peer):
                        act(copy)

                return carry

            lax.fori_loop(0, count, each, 0)

    for_heads(rounds, lambda copy: copy.start())

    if shared:
        def admit(peer, carry):
            pl.semaphore_signal(
                late_sem,
                inc=1,
                device_id={"frame": peer},
                device_id_type=pl.DeviceIdType.MESH,
            )
            return carry

        @pl.when(late)
        def _():
            lax.fori_loop(0, last, admit, 0)

        @pl.when(jnp.logical_not(late))
        def _():
            pl.semaphore_wait(late_sem, span)

        for_heads(late_rounds, lambda copy: copy.start())

    @pl.when(owner)
    def _():
        pltpu.make_async_copy(
            local.at[:, columns_of(my_head)],
            gathered.at[my_frame, pl.ds(my_row, rows), :],
            state_recv.at[my_frame],
        ).start()
        pltpu.make_async_copy(scale_out, scales.at[me], scale_recv.at[my_frame]).start()

    def send_part(place, part):
        target = place * span + part
        source = outgoing.at[place, pl.ds(pl.multiple_of(part * rows, rows), rows), :]
        goal = out_ref.at[0, :, columns_of(my_head)]
        remote = jnp.logical_or(target != me, nxt != segment)

        @pl.when(remote)
        def _():
            pltpu.make_async_remote_copy(
                src_ref=source,
                dst_ref=goal,
                send_sem=out_send,
                recv_sem=out_recv,
                device_id={"frame": target, "segment": nxt},
                device_id_type=pl.DeviceIdType.MESH,
            ).start()

        @pl.when(jnp.logical_not(remote))
        def _():
            pltpu.make_async_copy(source, goal, out_recv).start()

    def send_all():
        whole = jnp.logical_not(jnp.logical_or(lower, upper))
        paths = [
            (jnp.logical_and(whole, second_half), range(frames)),
            (jnp.logical_and(whole, jnp.logical_not(second_half)), range(frames)[::-1]),
        ]
        if shared:
            paths += [(lower, range(split)[::-1]), (upper, range(split, frames))]
        for chosen, places in paths:
            @pl.when(chosen)
            def _():
                def each(part, carry, skip):
                    for place in places:
                        if place >= skip:
                            send_part(place, part)
                    return carry

                lax.fori_loop(0, LEAD, lambda part, carry: each(part, carry, 1), 0)
                lax.fori_loop(LEAD, span, lambda part, carry: each(part, carry, 0), 0)


    def sent(count, send_sem):
        pieces = keys.at[pl.ds(0, count * rows), :]
        pltpu.make_async_copy(pieces, pieces, send_sem).wait()

    def sent_rows(count):
        sent(count, state_send)
        factors = scales.at[pl.ds(0, count)]
        pltpu.make_async_copy(factors, factors, scale_send).wait()

    def tokens_of(frame):
        return slice(frame * FRAME_TOK, (frame + 1) * FRAME_TOK)

    def mod_row(frame, kind):
        return mods[kind, pl.ds(level_ref[frame], 1), :]

    def project(frame):
        query_scale = (1.0 + mod_row(frame, 0)) * score_scale
        query_shift = mod_row(frame, 1) * score_scale
        key_scale, key_shift = 1.0 + mod_row(frame, 2), mod_row(frame, 3)
        value_scale, value_shift = 1.0 + mod_row(frame, 4), mod_row(frame, 5)
        queries = []
        for part in range(span):
            column = jnp.sum(
                jnp.where(diagonal, scales[frame * span + part], 0.0), axis=1, keepdims=True
            )
            inner = slice(part * rows, (part + 1) * rows)
            outer = slice(frame * FRAME_TOK + part * rows, frame * FRAME_TOK + (part + 1) * rows)
            wide = (
                (gathered[frame, inner, :].astype(jnp.float32) * column)
                .astype(jnp.bfloat16)
                .astype(jnp.float32)
            )
            keys[outer, :] = (wide * key_scale + key_shift).astype(jnp.bfloat16)
            values[outer, :] = (wide * value_scale + value_shift).astype(jnp.bfloat16)
            queries.append((wide * query_scale + query_shift).astype(jnp.bfloat16))
        return jnp.concatenate(queries, axis=0)

    def score(queries, other):
        return lax.dot_general(
            queries,
            keys[tokens_of(other), :],
            (((1,), (1,)), ((), ())),
            preferred_element_type=jnp.float32,
        )

    def attend(frame, queries, part, ready=()):
        queries = queries[part]
        scores = [
            ready[other][part] if other in ready else score(queries, other)
            for other in range(frame + 1)
        ]
        top = jnp.max(scores[frame], axis=-1, keepdims=True)
        for other in range(frame):
            peak = jnp.max(scores[other], axis=-1, keepdims=True)
            top = jnp.maximum(top, jnp.where(mask_ref[frame, other] == 1, peak, negative))
        summed, total = 0.0, 0.0
        for other in range(frame + 1):
            floor = top
            if other < frame:
                floor = top + jnp.where(mask_ref[frame, other] == 1, 0.0, -negative)
            weights = jnp.exp2(scores[other] - floor).astype(jnp.bfloat16)
            total += jnp.sum(weights.astype(jnp.float32), axis=-1, keepdims=True)
            summed += jnp.dot(
                weights, values[tokens_of(other), :], preferred_element_type=jnp.float32
            )
        attention = (summed / total).astype(jnp.bfloat16)
        done[frame, part, :] = (
            gathered[frame, part, :].astype(jnp.float32)
            + mod_row(frame, 6) * attention.astype(jnp.float32)
        ).astype(jnp.bfloat16)

    def source_of(place):
        return lax.rem(place + jnp.where(segment == segments - 1, offset_ref[0], 0), frames)

    lead = slice(0, LEAD * rows)
    trail = slice(LEAD * rows, FRAME_TOK)
    both = slice(0, FRAME_TOK)

    def send_lead():
        outgoing[0, lead, :] = done[source_of(0), lead, :]

        @pl.when(low == 0)
        def _():
            for part in range(LEAD):
                send_part(0, part)

    def send_rest():
        outgoing[0, trail, :] = done[source_of(0), trail, :]
        for place in range(1, frames):
            outgoing[place] = done[source_of(place)]
        send_all()

    def await_rows(frame):
        pltpu.make_async_copy(
            gathered.at[frame], gathered.at[frame], state_recv.at[frame]
        ).wait()
        arrived = scales.at[pl.ds(frame * span, span)]
        pltpu.make_async_copy(arrived, arrived, scale_recv.at[frame]).wait()

    def at_once():
        for frame in range(frames):
            await_rows(frame)
        held = [project(frame) for frame in range(frames)]
        for frame in range(frames):
            attend(frame, held[frame], both)
        send_lead()

    def last_apart(apart):
        for frame in range(frames - 1):
            await_rows(frame)
        held = [project(frame) for frame in range(frames - 1)]
        for frame in range(frames - 1):
            attend(frame, held[frame], both)
        await_rows(frames - 1)
        queries = project(frames - 1)
        attend(frames - 1, queries, lead if apart else both)
        send_lead()
        if apart:
            attend(frames - 1, queries, trail)

    def as_they_come(apart):
        for frame in range(frames - 2):
            await_rows(frame)
            attend(frame, project(frame), both)
        final = frames - 1
        await_rows(final)
        queries = project(final)
        ready = {
            other: score(queries, other) for other in range(frames) if other != final - 1
        }
        await_rows(final - 1)
        others = project(final - 1)
        first = lead if apart else both
        attend(final - 1, others, first)
        attend(final, queries, first, ready)
        send_lead()
        if apart:
            attend(final - 1, others, trail)
            attend(final, queries, trail, ready)

    @pl.when(owner)
    def _():
        mod_copy.wait()
        for copy in scalar_copies:
            copy.wait()
        middle = jnp.logical_and(second_half, jnp.logical_not(late))
        at_start = jnp.logical_or(early, late)
        rest = jnp.logical_not(jnp.logical_or(second_half, early))
        for chosen, run in (
            (at_start, at_once),
            (jnp.logical_and(middle, far), lambda: last_apart(True)),
            (jnp.logical_and(middle, jnp.logical_not(far)), lambda: last_apart(False)),
            (jnp.logical_and(rest, far), lambda: as_they_come(True)),
            (jnp.logical_and(rest, jnp.logical_not(far)), lambda: as_they_come(False)),
        ):
            @pl.when(chosen)
            def _():
                run()

        send_rest()

    kept = 1 if segments == 1 else 0

    @pl.when(owner)
    def _():
        sent_rows(copies - 1)

    @pl.when(jnp.logical_not(owner))
    def _():
        sent_rows(copies)

    whole = jnp.logical_and(owner, jnp.logical_not(jnp.logical_or(lower, upper)))
    for chosen, count in ((whole, frames), (lower, split), (upper, frames - split)):
        if shared or count == frames:
            @pl.when(chosen)
            def _():
                sent(count * span - kept, out_send)

    pltpu.make_async_copy(out_ref, out_ref, out_recv).wait()


def body(state, modulation, noise_level, frame_mask, offset):
    _, rows, width = state.shape
    _, levels, kinds, _ = modulation.shape
    devices = lax.axis_size("frame")
    segments = lax.axis_size("segment")
    heads = width // HEAD
    frames = devices * rows // FRAME_TOK
    tokens = devices * rows
    hbm = pl.BlockSpec(memory_space=pl.ANY)
    return pl.pallas_call(
        functools.partial(kernel, devices, segments, heads, frames, rows),
        out_shape=pltpu.VMEM(state.shape, jnp.bfloat16),
        in_specs=[hbm] * 5,
        out_specs=pl.BlockSpec(memory_space=pltpu.VMEM),
        scratch_shapes=[
            pltpu.SMEM(noise_level.shape, jnp.int32),
            pltpu.SMEM(frame_mask.shape, jnp.int32),
            pltpu.SMEM(offset.shape, jnp.int32),
            pltpu.VMEM((rows, width), jnp.bfloat16),
            pltpu.VMEM((frames, FRAME_TOK, HEAD), jnp.bfloat16),
            pltpu.VMEM((1, HEAD), jnp.float32),
            pltpu.VMEM((devices, 1, HEAD), jnp.float32),
            pltpu.VMEM((kinds, levels, HEAD), jnp.float32),
            pltpu.VMEM((tokens, HEAD), jnp.bfloat16),
            pltpu.VMEM((tokens, HEAD), jnp.bfloat16),
            pltpu.VMEM((frames, FRAME_TOK, HEAD), jnp.bfloat16),
            pltpu.VMEM((frames, FRAME_TOK, HEAD), jnp.bfloat16),
            pltpu.SemaphoreType.DMA((3,)),
            pltpu.SemaphoreType.DMA((1,)),
            pltpu.SemaphoreType.DMA,
            pltpu.SemaphoreType.DMA,
            pltpu.SemaphoreType.DMA((frames,)),
            pltpu.SemaphoreType.DMA,
            pltpu.SemaphoreType.DMA((frames,)),
            pltpu.SemaphoreType.DMA,
            pltpu.SemaphoreType.DMA,
            pltpu.SemaphoreType.REGULAR,
        ],
        compiler_params=pltpu.CompilerParams(has_side_effects=True, collective_id=0),
        name="denoise",
    )(noise_level, frame_mask, offset, state, jnp.swapaxes(modulation, 1, 2))


def solution(mesh):
    return jax.shard_map(
        body,
        mesh=mesh,
        in_specs=(P("segment", "frame", None), P("segment", None, None, None), P(), P(), P()),
        out_specs=P("segment", "frame", None),
        check_vma=False,
    )
```

```python
import functools
import math

import jax
import jax.numpy as jnp
from jax import lax
from jax.experimental import pallas as pl
from jax.experimental.pallas import tpu as pltpu
from jax.sharding import PartitionSpec as P

HEAD = 128
FRAME_TOK = 256

LEAD = 2

epsilon = 1e-06
negative = -1e30
score_scale = math.log2(math.e) / math.sqrt(HEAD)


def owner_plan(heads, devices, span):
    groups = heads // span
    if heads % span or span % 4 or (groups + 1) * span != devices or groups < 2:
        return [(0, 1, heads)], [], []
    last = devices - span
    pairs = span // 2
    order = [*range(1, groups), 0]
    evens = [(group * span, 2, pairs) for group in order]
    odds = [(group * span + 1, 2, pairs) for group in reversed(order)]
    return evens + odds, [], [(groups - 1, last, 2, pairs), (groups, last + 1, 2, pairs)]

def kernel(
    devices,
    segments,
    heads,
    frames,
    rows,
    level_hbm,
    mask_hbm,
    offset_hbm,
    state_ref,
    mod_ref,
    out_ref,
    level_ref,
    mask_ref,
    offset_ref,
    local,
    gathered,
    scale_out,
    scales,
    mods,
    keys,
    values,
    done,
    outgoing,
    scalar_sem,
    local_sem,
    mod_sem,
    state_send,
    state_recv,
    scale_send,
    out_send,
    out_recv,
    late_sem,
):
    me = lax.axis_index("frame")
    segment = lax.axis_index("segment")
    span = FRAME_TOK // rows
    width = heads * HEAD
    early_plan, late_plan, doubles = owner_plan(heads, devices, span)
    shared = bool(doubles)
    last = devices - span
    my_frame = lax.div(me, span)
    my_part = lax.rem(me, span)
    my_row = pl.multiple_of(my_part * rows, rows)

    def among(first, stride, count):
        place = me - first
        inside = jnp.logical_and(place >= 0, place < stride * count)
        if stride > 1:
            inside = jnp.logical_and(inside, lax.rem(place + stride * devices, stride) == 0)
        return inside, lax.div(place, stride)

    split = frames - 1
    owner, my_head, base, low, high = me < 0, 0, 0, 0, frames
    rounds, late_rounds = [], []
    for index, (first, stride, count) in enumerate(early_plan + late_plan):
        entry = (base, first, stride, count)
        (rounds if index < len(early_plan) else late_rounds).append(entry)
        inside, rank = among(first, stride, count)
        owner = jnp.logical_or(owner, inside)
        my_head = jnp.where(inside, base + rank, my_head)
        if index == 0:
            early = inside
        base += count
    leader, late = owner, me < 0
    lower, upper = me < 0, me < 0
    for index, first, stride, count in doubles:
        base, lower_first, lower_stride, _ = rounds[index]
        late_rounds.append((base, first, stride, count))
        inside, rank = among(first, stride, count)
        owner = jnp.logical_or(owner, inside)
        my_head = jnp.where(inside, base + rank, my_head)
        upper = jnp.logical_or(upper, inside)
        lower = jnp.logical_or(lower, among(lower_first, lower_stride, count)[0])
    if shared:
        late = me >= last
        leader = jnp.logical_not(late)
        low = jnp.where(upper, split, 0)
        high = jnp.where(lower, split, frames)
    copies = sum(entry[3] for entry in rounds + late_rounds)

    second_half = 2 * me >= devices
    far = my_part >= span - span // 4
    nxt = lax.rem(segment + 1, segments)
    barrier = pltpu.get_barrier_semaphore()

    def columns_of(head):
        return pl.ds(pl.multiple_of(head * HEAD, HEAD), HEAD)

    def greet(peer, peer_segment):
        pl.semaphore_signal(
            barrier,
            inc=1,
            device_id={"frame": peer, "segment": peer_segment},
            device_id_type=pl.DeviceIdType.MESH,
        )

    def greet_reader(index, carry):
        greet(index + jnp.where(index >= me, 1, 0), segment)
        return carry

    fetches = [
        pltpu.make_async_copy(
            state_ref.at[0, :, pl.ds(piece * (width // 1), width // 1)],
            local.at[:, pl.ds(piece * (width // 1), width // 1)],
            local_sem.at[piece],
        )
        for piece in range(1)
    ]
    for fetch in fetches:
        fetch.start()

    @pl.when(leader)
    def _():
        lax.fori_loop(0, devices - 1, greet_reader, 0)

    if shared:
        @pl.when(late)
        def _():
            lax.fori_loop(last, devices - 1, greet_reader, 0)

    if segments > 1:
        for _, first, stride, count in rounds + late_rounds:

            def greet_writer(index, carry):
                greet(first + stride * index, lax.rem(segment + segments - 1, segments))
                return carry

            lax.fori_loop(0, count, greet_writer, 0)

    scalar_copies = [
        pltpu.make_async_copy(source, place, scalar_sem.at[index])
        for index, (source, place) in enumerate(
            ((level_hbm, level_ref), (mask_hbm, mask_ref), (offset_hbm, offset_ref))
        )
    ]
    mod_copy = pltpu.make_async_copy(
        mod_ref.at[0, :, :, columns_of(my_head)], mods, mod_sem
    )

    @pl.when(owner)
    def _():
        mod_copy.start()
        for copy in scalar_copies:
            copy.start()

    for fetch in fetches:
        fetch.wait()
    widened = local[...].astype(jnp.float32)
    square_mean = jnp.sum(widened * widened, axis=-1, keepdims=True) * (1.0 / width)
    factor = lax.rsqrt(square_mean + epsilon)
    diagonal = lax.broadcasted_iota(jnp.int32, (rows, HEAD), 0) == lax.broadcasted_iota(
        jnp.int32, (rows, HEAD), 1
    )
    scale_out[...] = jnp.sum(
        jnp.where(diagonal, factor, 0.0), axis=0, keepdims=True
    )

    greetings = (last if shared else heads) - jnp.where(leader, 1, 0)
    if shared:
        greetings += jnp.where(late, span - 1, 0)
    if segments > 1:
        greetings += jnp.where(owner, devices, 0)
    pl.semaphore_wait(barrier, greetings)

    def copies_to(head, peer):
        return (
            pltpu.make_async_remote_copy(
                src_ref=local.at[:, columns_of(head)],
                dst_ref=gathered.at[my_frame, pl.ds(my_row, rows), :],
                send_sem=state_send,
                recv_sem=state_recv.at[my_frame],
                device_id={"frame": peer},
                device_id_type=pl.DeviceIdType.MESH,
            ),
            pltpu.make_async_remote_copy(
                src_ref=scale_out,
                dst_ref=scales.at[me],
                send_sem=scale_send,
                recv_sem=state_recv.at[my_frame],
                device_id={"frame": peer},
                device_id_type=pl.DeviceIdType.MESH,
            ),
        )

    def for_heads(chosen, act):
        for base, first, stride, count in chosen:
            turn = lax.rem(lax.div(me, 2) + 1, count)

            def each(index, carry):
                index += turn
                index = jnp.where(index >= count, index - count, index)
                peer = first + stride * index

                @pl.when(peer != me)
                def _():
                    for copy in copies_to(base + index, peer):
                        act(copy)

                return carry

            lax.fori_loop(0, count, each, 0)

    for_heads(rounds, lambda copy: copy.start())

    if shared:
        def admit(peer, carry):
            pl.semaphore_signal(
                late_sem,
                inc=1,
                device_id={"frame": peer},
                device_id_type=pl.DeviceIdType.MESH,
            )
            return carry

        @pl.when(late)
        def _():
            lax.fori_loop(0, last, admit, 0)

        @pl.when(jnp.logical_not(late))
        def _():
            pl.semaphore_wait(late_sem, span)

        for_heads(late_rounds, lambda copy: copy.start())

    @pl.when(owner)
    def _():
        pltpu.make_async_copy(
            local.at[:, columns_of(my_head)],
            gathered.at[my_frame, pl.ds(my_row, rows), :],
            state_recv.at[my_frame],
        ).start()
        pltpu.make_async_copy(scale_out, scales.at[me], state_recv.at[my_frame]).start()

    def send_part(place, part):
        target = place * span + part
        source = outgoing.at[place, pl.ds(pl.multiple_of(part * rows, rows), rows), :]
        goal = out_ref.at[0, :, columns_of(my_head)]
        remote = jnp.logical_or(target != me, nxt != segment)

        @pl.when(remote)
        def _():
            pltpu.make_async_remote_copy(
                src_ref=source,
                dst_ref=goal,
                send_sem=out_send,
                recv_sem=out_recv,
                device_id={"frame": target, "segment": nxt},
                device_id_type=pl.DeviceIdType.MESH,
            ).start()

        @pl.when(jnp.logical_not(remote))
        def _():
            pltpu.make_async_copy(source, goal, out_recv).start()

    def send_all():
        whole = jnp.logical_not(jnp.logical_or(lower, upper))
        paths = [
            (jnp.logical_and(whole, second_half), range(frames)),
            (jnp.logical_and(whole, jnp.logical_not(second_half)), range(frames)[::-1]),
        ]
        if shared:
            paths += [(lower, range(split)[::-1]), (upper, range(split, frames))]
        for chosen, places in paths:
            @pl.when(chosen)
            def _():
                def each(part, carry, skip):
                    for place in places:
                        if place >= skip:
                            send_part(place, part)
                    return carry

                lax.fori_loop(0, LEAD, lambda part, carry: each(part, carry, 1), 0)
                lax.fori_loop(LEAD, span, lambda part, carry: each(part, carry, 0), 0)


    def sent(count, send_sem):
        pieces = keys.at[pl.ds(0, count * rows), :]
        pltpu.make_async_copy(pieces, pieces, send_sem).wait()

    def sent_rows(count):
        sent(count, state_send)
        factors = scales.at[pl.ds(0, count)]
        pltpu.make_async_copy(factors, factors, scale_send).wait()

    def tokens_of(frame):
        return slice(frame * FRAME_TOK, (frame + 1) * FRAME_TOK)

    def mod_row(frame, kind):
        return mods[kind, pl.ds(level_ref[frame], 1), :]

    def project(frame):
        query_scale = (1.0 + mod_row(frame, 0)) * score_scale
        query_shift = mod_row(frame, 1) * score_scale
        key_scale, key_shift = 1.0 + mod_row(frame, 2), mod_row(frame, 3)
        value_scale, value_shift = 1.0 + mod_row(frame, 4), mod_row(frame, 5)
        queries = []
        for part in range(span):
            column = jnp.sum(
                jnp.where(diagonal, scales[frame * span + part], 0.0), axis=1, keepdims=True
            )
            inner = slice(part * rows, (part + 1) * rows)
            outer = slice(frame * FRAME_TOK + part * rows, frame * FRAME_TOK + (part + 1) * rows)
            wide = (
                (gathered[frame, inner, :].astype(jnp.float32) * column)
                .astype(jnp.bfloat16)
                .astype(jnp.float32)
            )
            keys[outer, :] = (wide * key_scale + key_shift).astype(jnp.bfloat16)
            values[outer, :] = (wide * value_scale + value_shift).astype(jnp.bfloat16)
            queries.append((wide * query_scale + query_shift).astype(jnp.bfloat16))
        return jnp.concatenate(queries, axis=0)

    def score(queries, other):
        return lax.dot_general(
            queries,
            keys[tokens_of(other), :],
            (((1,), (1,)), ((), ())),
            preferred_element_type=jnp.float32,
        )

    def attend(frame, queries, part, ready=()):
        queries = queries[part]
        scores = [
            ready[other][part] if other in ready else score(queries, other)
            for other in range(frame + 1)
        ]
        top = jnp.max(scores[frame], axis=-1, keepdims=True)
        for other in range(frame):
            peak = jnp.max(scores[other], axis=-1, keepdims=True)
            top = jnp.maximum(top, jnp.where(mask_ref[frame, other] == 1, peak, negative))
        summed, total = 0.0, 0.0
        for other in range(frame + 1):
            floor = top
            if other < frame:
                floor = top + jnp.where(mask_ref[frame, other] == 1, 0.0, -negative)
            weights = jnp.exp2(scores[other] - floor).astype(jnp.bfloat16)
            total += jnp.sum(weights.astype(jnp.float32), axis=-1, keepdims=True)
            summed += jnp.dot(
                weights, values[tokens_of(other), :], preferred_element_type=jnp.float32
            )
        attention = (summed / total).astype(jnp.bfloat16)
        done[frame, part, :] = (
            gathered[frame, part, :].astype(jnp.float32)
            + mod_row(frame, 6) * attention.astype(jnp.float32)
        ).astype(jnp.bfloat16)

    def source_of(place):
        return lax.rem(place + jnp.where(segment == segments - 1, offset_ref[0], 0), frames)

    lead = slice(0, LEAD * rows)
    trail = slice(LEAD * rows, FRAME_TOK)
    both = slice(0, FRAME_TOK)

    def send_lead():
        outgoing[0, lead, :] = done[source_of(0), lead, :]

        @pl.when(low == 0)
        def _():
            for part in range(LEAD):
                send_part(0, part)

    def send_rest():
        outgoing[0, trail, :] = done[source_of(0), trail, :]
        for place in range(1, frames):
            outgoing[place] = done[source_of(place)]
        send_all()

    def await_rows(frame):
        arrived = keys.at[pl.ds(0, span * (rows + 2)), :]
        pltpu.make_async_copy(arrived, arrived, state_recv.at[frame]).wait()

    def at_once(apart):
        for frame in range(frames):
            await_rows(frame)
        held = [project(frame) for frame in range(frames)]
        for frame in range(frames):
            attend(frame, held[frame], lead if apart else both)
        send_lead()
        if apart:
            for frame in range(frames):
                attend(frame, held[frame], trail)

    def last_apart(apart):
        for frame in range(frames - 1):
            await_rows(frame)
        held = [project(frame) for frame in range(frames - 1)]
        for frame in range(frames - 1):
            attend(frame, held[frame], both)
        await_rows(frames - 1)
        queries = project(frames - 1)
        attend(frames - 1, queries, lead if apart else both)
        send_lead()
        if apart:
            attend(frames - 1, queries, trail)

    def as_they_come(apart):
        for frame in range(frames - 2):
            await_rows(frame)
            attend(frame, project(frame), both)
        final = frames - 1
        await_rows(final)
        queries = project(final)
        ready = {
            other: score(queries, other) for other in range(frames) if other != final - 1
        }
        await_rows(final - 1)
        others = project(final - 1)
        first = lead if apart else both
        attend(final - 1, others, first)
        attend(final, queries, first, ready)
        send_lead()
        if apart:
            attend(final - 1, others, trail)
            attend(final, queries, trail, ready)

    @pl.when(owner)
    def _():
        mod_copy.wait()
        for copy in scalar_copies:
            copy.wait()
        even = lax.rem(me, 2) == 0
        middle = jnp.logical_and(second_half, jnp.logical_not(late))
        rest = jnp.logical_not(jnp.logical_or(second_half, early))
        for chosen, run, apart in (
            (jnp.logical_or(early, late), at_once, False),
            (jnp.logical_and(middle, even), at_once, None),
            (jnp.logical_and(middle, jnp.logical_not(even)), last_apart, None),
            (rest, as_they_come, None),
        ):
            for split_rows in (False, True) if apart is None else (apart,):
                ways = far if split_rows else jnp.logical_not(far)
                here = chosen if apart is not None else jnp.logical_and(chosen, ways)

                @pl.when(here)
                def _():
                    run(split_rows)

        send_rest()

    kept = 1 if segments == 1 else 0

    @pl.when(owner)
    def _():
        sent_rows(copies - 1)

    @pl.when(jnp.logical_not(owner))
    def _():
        sent_rows(copies)

    whole = jnp.logical_and(owner, jnp.logical_not(jnp.logical_or(lower, upper)))
    for chosen, count in ((whole, frames), (lower, split), (upper, frames - split)):
        if shared or count == frames:
            @pl.when(chosen)
            def _():
                sent(count * span - kept, out_send)

    pltpu.make_async_copy(out_ref, out_ref, out_recv).wait()


def body(state, modulation, noise_level, frame_mask, offset):
    _, rows, width = state.shape
    _, levels, kinds, _ = modulation.shape
    devices = lax.axis_size("frame")
    segments = lax.axis_size("segment")
    heads = width // HEAD
    frames = devices * rows // FRAME_TOK
    tokens = devices * rows
    hbm = pl.BlockSpec(memory_space=pl.ANY)
    return pl.pallas_call(
        functools.partial(kernel, devices, segments, heads, frames, rows),
        out_shape=pltpu.VMEM(state.shape, jnp.bfloat16),
        in_specs=[hbm] * 5,
        out_specs=pl.BlockSpec(memory_space=pltpu.VMEM),
        scratch_shapes=[
            pltpu.SMEM(noise_level.shape, jnp.int32),
            pltpu.SMEM(frame_mask.shape, jnp.int32),
            pltpu.SMEM(offset.shape, jnp.int32),
            pltpu.VMEM((rows, width), jnp.bfloat16),
            pltpu.VMEM((frames, FRAME_TOK, HEAD), jnp.bfloat16),
            pltpu.VMEM((1, HEAD), jnp.float32),
            pltpu.VMEM((devices, 1, HEAD), jnp.float32),
            pltpu.VMEM((kinds, levels, HEAD), jnp.float32),
            pltpu.VMEM((tokens, HEAD), jnp.bfloat16),
            pltpu.VMEM((tokens, HEAD), jnp.bfloat16),
            pltpu.VMEM((frames, FRAME_TOK, HEAD), jnp.bfloat16),
            pltpu.VMEM((frames, FRAME_TOK, HEAD), jnp.bfloat16),
            pltpu.SemaphoreType.DMA((3,)),
            pltpu.SemaphoreType.DMA((1,)),
            pltpu.SemaphoreType.DMA,
            pltpu.SemaphoreType.DMA,
            pltpu.SemaphoreType.DMA((frames,)),
            pltpu.SemaphoreType.DMA,
            pltpu.SemaphoreType.DMA,
            pltpu.SemaphoreType.DMA,
            pltpu.SemaphoreType.REGULAR,
        ],
        compiler_params=pltpu.CompilerParams(has_side_effects=True, collective_id=0),
        name="denoise",
    )(noise_level, frame_mask, offset, state, jnp.swapaxes(modulation, 1, 2))


def solution(mesh):
    return jax.shard_map(
        body,
        mesh=mesh,
        in_specs=(P("segment", "frame", None), P("segment", None, None, None), P(), P(), P()),
        out_specs=P("segment", "frame", None),
        check_vma=False,
    )
```
